512 devices in a mesh: groups: 2 (over y), ep: 128 (over z, x), role: 2 (over core).
Axes of the slice: x: 8, y: 2, z: 16, core: 2. Of those that a mesh axis runs over, the one named last changes fastest.
The devices are a block of a 8x8x16 slice.
Arguments:
- residual: bfloat16 [3072, 2880], P(('groups', 'ep', 'role')), parts along dimension 0, may hold values from -1.796875 to 1.796875
- queries: bfloat16 [3072, 2880], P(('groups', 'ep', 'role')), parts along dimension 0, may hold values from -150 to 150
- key_new: bfloat16 [3072, 320], P(('groups', 'ep', 'role')), parts along dimension 0, may hold values from -6 to 6
- value_new: bfloat16 [3072, 320], P(('groups', 'ep', 'role')), parts along dimension 0, may hold values from -6 to 6
- key_cache: bfloat16 [3072, 128, 320], P(('groups', 'ep', 'role')), parts along dimension 0, may hold values from -6 to 6
- value_cache: bfloat16 [3072, 128, 320], P(('groups', 'ep', 'role')), parts along dimension 0, may hold values from -6 to 6
- lengths: int32 [3072], P(('groups', 'ep', 'role')), parts along dimension 0, may hold values from 1 to 512
- sink_logits: float32 [45], replicated, may hold values from -6 to 6
- norm_gain: float32 [2880], replicated, may hold values from 0.1 to 1.9
- route_ids: int32 [3072, 4], P(('groups', 'ep')), parts along dimension 0, may hold values from 0 to 63, all different within a row; in each aligned block of 12 rows (0 to 11, 12 to 23, ...) at most 2 rows name the same one
- route_logits: float32 [3072, 4], P(('groups', 'ep')), parts along dimension 0, may hold values from -1 to 1
- up_weight: bfloat16 [2880, 92160], P(None, ('ep', 'role')), may hold values from -0.109375 to 0.109375
- down_weight: bfloat16 [92160, 2880], P(('ep', 'role')), may hold values from -0.15625 to 0.15625
Outputs:
- layer_out: bfloat16 [3072, 2880], P(('groups', 'ep', 'role')), parts along dimension 0
The draws below stay inside these ranges and needn't reach their ends.
There are 2 independent parts, one for each index of `groups`. The reference program is written for one: setup_inputs(seed, part) draws one part's arguments, and reference() takes and returns one part's arrays. A program takes and returns all parts, laid end to end along the dimension named above; an argument that names none is the same for every part. Nothing has to cross between parts.
Inputs may be any that keep to these rules, and one draw needn't show every extreme that they name: `route_ids`: in each aligned block of 12 rows (the tokens of one index of ep) no expert is named more than 2 times, a bound that some block reaches.
All inputs are finite; a program needn't handle non-finite values.
Results may differ from the reference program's by a relative error of at most 0.0095.
Values may be sent and summed in bfloat16 or wider, within the bound.
A program may use at most 64 MiB of HBM per device.

```python
import math
import jax
import jax.numpy as jnp
import numpy as np
from jax import lax

D = 2880
HD = 64
QH = 45
KVH = 5
WIN = 128
TOPK = 4
HID_DEV = 360
TOK_DEV = 6
CAP = 2
EXPERTS = 64
FF = 1440
TOKENS = 1536
N_EP = 128
N_ROLE = 2


def draw_queries(key, part):
    base = jax.random.normal(jax.random.fold_in(key, 11), (TOKENS, QH * HD), jnp.float32)
    return jnp.clip(base, -6.0, 6.0).astype(jnp.bfloat16)


def with_ends(array, key, least, high):
    index_at = [jax.random.randint(jax.random.fold_in(key, axis), (), 0, length) for axis, length in enumerate(array.shape)]
    widest = array.shape.index(max(array.shape))
    neighbour = index_at[:widest] + [(index_at[widest] + 1) % array.shape[widest]] + index_at[widest + 1:]
    return array.at[tuple(index_at)].set(least).at[tuple(neighbour)].set(high)


def levels(stream_key, shape, cuts, low, high):
    loudness = 1.0
    for dim, blocks in cuts:
        draws = jax.random.uniform(jax.random.fold_in(jax.random.fold_in(stream_key, 6), dim), (blocks,), jnp.float32, low / len(cuts), high / len(cuts))
        loudness = loudness * jnp.repeat(jnp.exp(draws), shape[dim] // blocks).reshape((-1,) + (1,) * (len(shape) - 1 - dim))
    return loudness


def assign_block(key, own, number, rows, count, top, limit, lean):
    ranking = jax.random.permutation(key, count)
    packed, common = portions_of(count, rows * top, limit, lean, True), portions_of(count, rows * top, limit, lean, False)
    places = jnp.arange(count)

    def named(sizes, rotation):
        used = int((sizes > 0).sum())
        fixed = max(1, used // 4)
        moved = fixed + (places - fixed + rotation * (used - fixed)) % max(1, count - fixed)
        return jnp.zeros((count,), jnp.int32).at[ranking[jnp.where(places < fixed, places, moved)]].set(jnp.asarray(sizes, jnp.int32))

    sizes = jnp.where(number % 4 == 0, named(packed, number // 4), named(common, number - number // 4 - 1))
    mixed = jax.random.permutation(jax.random.fold_in(own, 3), count)
    donor, taker = mixed[0:count // 2 * 2:2], mixed[1:count // 2 * 2:2]
    margin = jnp.minimum(sizes[donor] - 1, limit - sizes[taker]) // 2
    margin = jnp.where((donor == ranking[0]) | (taker == ranking[0]) | (sizes[taker] == 0), 0, jnp.maximum(margin, 0))
    moved = jax.random.randint(jax.random.fold_in(own, 4), (count // 2,), 0, 1 << 20) % (margin + 1)
    sizes = sizes.at[donor].add(-moved).at[taker].add(moved)
    items = jnp.searchsorted(jnp.cumsum(sizes), jnp.arange(rows * top), side="right").astype(jnp.int32)
    table = items.reshape(top, rows).T
    table = table[jax.random.permutation(jax.random.fold_in(own, 1), rows)]
    rotation = jax.random.randint(jax.random.fold_in(own, 2), (rows, 1), 0, top)
    return jnp.take_along_axis(table, (jnp.arange(top)[None, :] + rotation) % top, axis=1)


def portions_of(number_of, total, most, slope, full):
    loads = [(1 << 20) // math.isqrt(standing ** slope) + 1 for standing in range(1, number_of + 1)]
    largest = most if full else min(most, max(-(-total // number_of), total * loads[0] // sum(loads)))
    least = 1 if total - largest >= number_of - 1 else 0
    holding, surplus = [largest] + [least] * (number_of - 1), total - largest - least * (number_of - 1)
    while surplus > 0:
        free = [i for i in range(1, number_of) if holding[i] < largest] or [i for i in range(1, number_of) if holding[i] < most]
        whole, budget = sum([loads[i] for i in free]), surplus
        for i in free:
            more = min(most - holding[i], max(1, budget * loads[i] // whole), surplus)
            holding[i] = holding[i] + more
            surplus = surplus - more
    return np.array(holding)


def noise(stream_key, shape, scale, reach, split=(), kind=jnp.bfloat16):
    array = scale * jax.random.normal(stream_key, shape, jnp.float32)
    if split:
        array = array * levels(stream_key, shape, split, -0.22, 0.18)
    return jnp.clip(array, -reach, reach).astype(kind)


def setup_inputs(seed: int = 0, part: int = 0) -> dict:
    key_of = jax.random.split(jax.random.key(seed), 14)
    part_keys = jax.random.split(jax.random.fold_in(key_of[13], part), 14)
    residual = noise(part_keys[0], (TOKENS, D), 0.3, 1.796875, ((0, 256),))
    queries = draw_queries(jax.random.fold_in(jax.random.fold_in(key_of[13], part), 71), part)
    key_new = noise(part_keys[2], (TOKENS, KVH * HD), 1.0, 6.0, ((0, 256),))
    value_new = noise(part_keys[3], (TOKENS, KVH * HD), 1.0, 6.0, ((0, 256),))
    key_cache = noise(part_keys[4], (TOKENS, WIN, KVH * HD), 1.0, 6.0, ((0, 256),))
    value_cache = noise(part_keys[5], (TOKENS, WIN, KVH * HD), 1.0, 6.0, ((0, 256),))
    lengths = with_ends(jax.random.randint(part_keys[6], (TOKENS,), 1, 4 * WIN + 1), jax.random.fold_in(part_keys[6], 1), 1, 4 * WIN).astype(jnp.int32)
    sink_logits = noise(key_of[7], (QH,), 1.5, 6.0, (), jnp.float32)
    norm_gain = jnp.clip(1.0 + 0.18 * jax.random.normal(key_of[8], (D,), jnp.float32), 0.1, 1.9)
    route_ids_keys = jax.random.split(jax.random.fold_in(part_keys[9], 1), TOKENS // (2 * TOK_DEV))
    route_ids_turns = jax.random.permutation(jax.random.fold_in(part_keys[9], 3), TOKENS // (2 * TOK_DEV))
    route_ids = jax.vmap(lambda own, number: assign_block(jax.random.fold_in(part_keys[9], 2), own, number, 2 * TOK_DEV, EXPERTS, TOPK, CAP, 2))(route_ids_keys, route_ids_turns).reshape((TOKENS, TOPK))
    route_logits = jnp.clip(jax.random.uniform(part_keys[10], (TOKENS, TOPK), jnp.float32, -1.0, 1.0) * levels(part_keys[10], (TOKENS, TOPK), ((0, 128),), -0.4, 0.0), -1.0, 1.0)
    up_weight = noise(key_of[11], (D, EXPERTS * FF), D ** -0.5, 0.109375, ((1, 256),))
    down_weight = noise(key_of[12], (EXPERTS * FF, D), FF ** -0.5, 0.15625, ((0, 256),))
    return dict(residual=residual, queries=queries, key_new=key_new, value_new=value_new, key_cache=key_cache, value_cache=value_cache, lengths=lengths, sink_logits=sink_logits, norm_gain=norm_gain, route_ids=route_ids, route_logits=route_logits, up_weight=up_weight, down_weight=down_weight)


def attention(queries, key_new, value_new, key_cache, value_cache, lengths, sink_logits):
    request_count = queries.shape[0]
    window = key_cache.shape[1]
    heads_kv = key_new.shape[1] // HD
    group_size = queries.shape[1] // (heads_kv * HD)
    query_heads = queries.astype(jnp.float32).reshape(request_count, heads_kv, group_size, HD)
    cached_keys = key_cache.astype(jnp.float32).reshape(request_count, window, heads_kv, HD)
    cached_values = value_cache.astype(jnp.float32).reshape(request_count, window, heads_kv, HD)
    fresh_key = key_new.astype(jnp.float32).reshape(request_count, heads_kv, HD)
    fresh_value = value_new.astype(jnp.float32).reshape(request_count, heads_kv, HD)
    score_scale = HD ** (-0.5)
    cached = jnp.einsum('tkgd,tskd->tkgs', query_heads, cached_keys) * score_scale
    fresh_score = jnp.einsum('tkgd,tkd->tkg', query_heads, fresh_key) * score_scale
    newest = lengths[:, None] - 1
    slot_index = jnp.arange(window, dtype=jnp.int32)[None, :]
    position = newest - jnp.mod(newest - slot_index, window)
    visible = (position >= 0) & (position >= lengths[:, None] - window + 1)
    cached = jnp.where(visible[:, None, None, :], cached, -1e+30)
    sink_logit = sink_logits.reshape(1, heads_kv, group_size)
    highest = jnp.maximum(jnp.maximum(lax.optimization_barrier(jnp.max(cached, -1)), fresh_score), sink_logit)
    weights = jnp.exp(cached - highest[..., None])
    fresh_weight = jnp.exp(fresh_score - highest)
    denominator = lax.optimization_barrier(jnp.sum(weights, -1)) + fresh_weight + jnp.exp(sink_logit - highest)
    cache_probs = (weights / denominator[..., None]).astype(jnp.bfloat16)
    fresh_prob = (fresh_weight / denominator).astype(jnp.bfloat16)
    context = jnp.einsum('tkgs,tskd->tkgd', cache_probs.astype(jnp.float32), cached_values)
    context = context + fresh_prob.astype(jnp.float32)[..., None] * fresh_value[:, :, None, :]
    return context.reshape(request_count, -1)

def reference(residual, queries, key_new, value_new, key_cache, value_cache, lengths, sink_logits, norm_gain, route_ids, route_logits, up_weight, down_weight):
    context = attention(queries, key_new, value_new, key_cache, value_cache, lengths, sink_logits)
    hidden_state = residual.astype(jnp.float32) + context
    normed = (hidden_state * lax.rsqrt(lax.optimization_barrier(jnp.mean(hidden_state * hidden_state, -1, keepdims=True)) + 1e-05) * norm_gain).astype(jnp.bfloat16)
    gate_weights = jax.nn.softmax(route_logits, axis=-1)
    request_count, pick_count = route_ids.shape
    blocks = N_EP
    block_ids = route_ids.reshape(blocks, -1)
    onehot = (block_ids[..., None] == jnp.arange(EXPERTS, dtype=jnp.int32)).astype(jnp.int32)
    earlier = jnp.cumsum(onehot, axis=1) - onehot
    slot_number = lax.optimization_barrier(jnp.sum(earlier * onehot, -1))
    slot_place = (jnp.arange(blocks, dtype=jnp.int32)[:, None] * CAP + slot_number).reshape(-1).astype(jnp.int32)
    expert_flat = route_ids.reshape(-1).astype(jnp.int32)
    token_flat = jnp.repeat(jnp.arange(request_count, dtype=jnp.int32), pick_count)
    index_table = jnp.zeros((EXPERTS, blocks * CAP), jnp.int32).at[expert_flat, slot_place].set(token_flat)
    gate_table = jnp.zeros((EXPERTS, blocks * CAP), jnp.float32).at[expert_flat, slot_place].set(gate_weights.reshape(-1))
    quarters = 2 * N_ROLE
    up_stack = up_weight.reshape(D, EXPERTS, FF).transpose(1, 0, 2)
    down_stack = down_weight.reshape(EXPERTS, quarters, HID_DEV, D)

    def expert_step(running, inputs):
        row_index, row_gate, up_block, down_block = inputs
        gathered = normed[row_index]
        activation = jax.nn.silu(jnp.dot(gathered, up_block, preferred_element_type=jnp.float32)).astype(jnp.bfloat16)
        split_act = activation.reshape(-1, quarters, HID_DEV).astype(jnp.float32)
        partials = jnp.einsum('rqh,qhd->rqd', split_act, down_block.astype(jnp.float32)).astype(jnp.bfloat16)
        summed = lax.optimization_barrier(jnp.sum(partials.astype(jnp.float32), axis=1)) * row_gate[:, None]
        return (running.at[row_index].add(summed), None)
    expert_out, _ = lax.scan(expert_step, jnp.zeros((request_count, D), jnp.float32), (index_table, gate_table, up_stack, down_stack))
    return (hidden_state + expert_out).astype(jnp.bfloat16)
```

```python
import functools

import jax
import jax.numpy as jnp
from jax import lax
from jax.experimental import pallas as pl
from jax.experimental.pallas import tpu as pltpu
from jax.sharding import PartitionSpec as P

HD = 64
ROWS = 8
TILE = 16
MESH = pl.DeviceIdType.MESH
BF16 = jnp.bfloat16
F32 = jnp.float32


def attention(queries, key_new, value_new, key_cache, value_cache, lengths, sink_logits):
    request_count = queries.shape[0]
    window = key_cache.shape[1]
    heads_kv = key_new.shape[1] // HD
    group_size = queries.shape[1] // (heads_kv * HD)
    query_heads = queries.reshape(request_count, heads_kv, group_size, HD)
    cached_keys = key_cache.reshape(request_count, window, heads_kv, HD)
    cached_values = value_cache.reshape(request_count, window, heads_kv, HD)
    fresh_key = key_new.reshape(request_count, heads_kv, HD)
    fresh_value = value_new.reshape(request_count, heads_kv, HD)
    score_scale = HD ** (-0.5)
    cached = (
        jnp.einsum("tkgd,tskd->tkgs", query_heads, cached_keys, preferred_element_type=jnp.float32)
        * score_scale
    )
    fresh_score = (
        jnp.einsum("tkgd,tkd->tkg", query_heads, fresh_key, preferred_element_type=jnp.float32)
        * score_scale
    )
    newest = lengths[:, None] - 1
    slot_index = jnp.arange(window, dtype=jnp.int32)[None, :]
    position = newest - jnp.mod(newest - slot_index, window)
    visible = (position >= 0) & (position >= lengths[:, None] - window + 1)
    cached = jnp.where(visible[:, None, None, :], cached, -1e30)
    sink_logit = sink_logits.reshape(1, heads_kv, group_size)
    highest = jnp.maximum(jnp.maximum(jnp.max(cached, -1), fresh_score), sink_logit)
    weights = jnp.exp(cached - highest[..., None])
    fresh_weight = jnp.exp(fresh_score - highest)
    denominator = jnp.sum(weights, -1) + fresh_weight + jnp.exp(sink_logit - highest)
    cache_probs = (weights / denominator[..., None]).astype(jnp.bfloat16)
    fresh_prob = (fresh_weight / denominator).astype(jnp.bfloat16)
    context = jnp.einsum(
        "tkgs,tskd->tkgd", cache_probs, cached_values, preferred_element_type=jnp.float32
    )
    context = (
        context
        + fresh_prob.astype(jnp.float32)[..., None] * fresh_value.astype(jnp.float32)[:, :, None, :]
    )
    return context.reshape(request_count, -1)


def ring_offsets(n):
    offsets = [0]
    for d in range(1, n // 2 + 1):
        offsets += [d] if 2 * d == n else [d, -d]
    opposite = [next(b for b, o in enumerate(offsets) if (o + offsets[a]) % n == 0) for a in range(n)]
    return offsets, opposite


def moe_kernel(
    nx, nz, capacity, width, chunk,
    normed, table, up_hbm, down_hbm, out,
    up, down, gath, tabs, packed, rows, part, part_in, half_out, half_in, back, returned, mixed, final,
    weight_sem, tab_s, tab_r, gath_s, gath_r, out_s, out_r, fwd_s, fwd_r, back_s, back_r, fin_s, fin_r,
):
    ep, role = lax.axis_index("ep"), lax.axis_index("role")
    z, x = ep // nx, ep % nx
    half = x % 2
    mine = x * 2 + role
    quarter = half * 2 + role
    sibling = {"ep": ep, "role": 1 - role}
    pair = {"ep": ep + 1 - 2 * half, "role": role}
    qw = packed.shape[-1]
    block = nx * capacity
    offsets, opposite = ring_offsets(nz)
    plane = [(d, f) for d in range(nx) for f in range(2) if d or f]

    def in_plane(d, f):
        other_x, other_role = (x + d) % nx, (role + f) % 2
        return other_x, other_role, {"ep": z * nx + other_x, "role": other_role}

    def along_z(k):
        return {"ep": ((z + offsets[k] + nz) % nz) * nx + x, "role": role}

    def send(src, dst, ssem, rsem, device):
        copy = pltpu.make_async_remote_copy(
            src_ref=src, dst_ref=dst, send_sem=ssem, recv_sem=rsem, device_id=device, device_id_type=MESH
        )
        copy.start()
        return copy

    sent = []
    barrier = pltpu.get_barrier_semaphore()
    for d, f in plane:
        pl.semaphore_signal(barrier, inc=1, device_id=in_plane(d, f)[2], device_id_type=MESH)
    for k in range(1, nz):
        pl.semaphore_signal(barrier, inc=1, device_id=along_z(k), device_id_type=MESH)
    up_copy = pltpu.make_async_copy(up_hbm, up.at[pl.ds(0, width), :], weight_sem.at[0])
    up_copy.start()
    down_copy = pltpu.make_async_copy(down_hbm, down, weight_sem.at[1])
    down_copy.start()
    pl.semaphore_wait(barrier, len(plane) + nz - 1)

    tab_copies, gath_copies = [], []
    for n, (d, f) in enumerate(plane):
        other_x, other_role, device = in_plane(d, f)
        if f == 0:
            tab_copies.append(send(table.at[other_x // 2], tabs.at[x], tab_s.at[d], tab_r.at[d], device))
        wanted = (other_x % 2) * 2 + other_role
        gath_copies.append(send(normed.at[wanted], gath.at[mine], gath_s.at[n], gath_r.at[n], device))
    up[pl.ds(width, 4 * qw - width), :] = jnp.zeros((4 * qw - width, up.shape[1]), BF16)
    gath[mine] = normed[quarter]
    tabs[x] = table[x // 2]
    last = width - 3 * qw
    clear = last // 128 * 128
    for h in (1,):
        part[h, 1, :, :, clear:] = jnp.zeros((nz, block, qw - clear), BF16)
    for copy in tab_copies:
        copy.wait_recv()
    lanes = tabs.shape[-1] // 2
    codes = jnp.sum(tabs[...].astype(F32), axis=0)
    slots, gates = codes[:, :lanes], codes[:, lanes:]
    row = lax.broadcasted_iota(jnp.int32, (nz, block, lanes), 1)
    col = lax.broadcasted_iota(jnp.int32, (nz, block, lanes), 2)
    hit = (col // (2 * ROWS) == row // capacity) & (
        jnp.broadcast_to(slots[:, None, :], (nz, block, lanes)) == (row % capacity + 1).astype(F32)
    )
    choose = jnp.where(hit, 1.0, 0.0).astype(BF16).reshape(nz * block, lanes)
    blend = jnp.where(hit, jnp.broadcast_to(gates[:, None, :], (nz, block, lanes)), 0.0).astype(BF16)
    blend = blend.reshape(nz * block, lanes)
    for copy in gath_copies:
        copy.wait_recv()
    tokens = gath[...].reshape(2 * nx * ROWS, qw)
    if tokens.shape[0] < lanes:
        tokens = jnp.concatenate([tokens, jnp.zeros((lanes - tokens.shape[0], qw), BF16)], axis=0)
    packed[...] = jnp.dot(choose, tokens, preferred_element_type=F32).astype(BF16).reshape(nz, block, qw)

    out_copies = {}
    for k in range(1, nz):
        to = opposite[k]
        out_copies[k] = send(packed.at[k], rows.at[quarter, to], out_s.at[k], out_r.at[to], along_z(k))
    rows[quarter, 0] = packed[0]
    back_copies = {}
    live = {}
    chunks = nz // chunk

    def span(c):
        return pl.ds(c * chunk, chunk)

    def stage_in(c):
        for k in range(c * chunk, (c + 1) * chunk):
            if k:
                out_copies[opposite[k]].wait_recv()
        mine_rows = rows.at[quarter, span(c)]
        live["pair", c] = send(mine_rows, mine_rows, fwd_s.at[0, c], fwd_r.at[0, c], pair)
        live["sib", c] = send(mine_rows, mine_rows, fwd_s.at[1, c], fwd_r.at[1, c], sibling)

    def stage_relay(c):
        live["pair", c].wait_recv()
        their_rows = rows.at[(1 - half) * 2 + role, span(c)]
        live["relay", c] = send(their_rows, their_rows, fwd_s.at[2, c], fwd_r.at[2, c], sibling)

    def stage_ffn(c):
        live["sib", c].wait_recv()
        live["relay", c].wait_recv()
        if c == 0:
            up_copy.wait()
        total = None
        for q in range(4):
            piece = rows[q, c * chunk : (c + 1) * chunk].reshape(chunk * block, qw)
            term = jnp.dot(piece, up[q * qw : (q + 1) * qw, :], preferred_element_type=F32)
            total = term if total is None else total + term
        active = (total / (1.0 + jnp.exp(-total))).astype(BF16)
        if c == 0:
            down_copy.wait()
        for q in range(4):
            w = min(qw, width - q * qw)
            value = jnp.dot(active, down[:, q * qw : q * qw + w], preferred_element_type=F32).astype(BF16)
            part[q // 2, q % 2, c * chunk : (c + 1) * chunk, :, :w] = value.reshape(chunk, block, w)
        live["part", c] = send(
            part.at[:, 1 - role, span(c)], part_in.at[:, span(c)], fwd_s.at[3, c], fwd_r.at[3, c], sibling
        )

    def stage_half(c):
        live["part", c].wait_recv()
        at = slice(c * chunk, (c + 1) * chunk)
        half_out[at] = (part[1 - half, role, at].astype(F32) + part_in[1 - half, at].astype(F32)).astype(BF16)
        live["half", c] = send(half_out.at[span(c)], half_in.at[span(c)], fwd_s.at[4, c], fwd_r.at[4, c], pair)

    def stage_back(c):
        live["half", c].wait_recv()
        at = slice(c * chunk, (c + 1) * chunk)
        back[at] = (
            part[half, role, at].astype(F32) + part_in[half, at].astype(F32) + half_in[at].astype(F32)
        ).astype(BF16)
        for k in range(c * chunk, (c + 1) * chunk):
            if k == 0:
                returned[0] = back[0]
            else:
                to = opposite[k]
                back_copies[k] = send(back.at[k], returned.at[to], back_s.at[k], back_r.at[to], along_z(k))

    for t in range(chunks + 2):
        if t < chunks:
            stage_in(t)
        if 0 <= t - 1 < chunks:
            stage_relay(t - 1)
            stage_ffn(t - 1)
            stage_half(t - 1)
        if 0 <= t - 2 < chunks:
            stage_back(t - 2)

    for k in range(1, nz):
        back_copies[opposite[k]].wait_recv()
    mix = lax.dot_general(
        blend, returned[...].reshape(nz * block, qw), (((0,), (0,)), ((), ())), preferred_element_type=F32
    )
    mixed[...] = mix[: 2 * nx * ROWS].astype(BF16).reshape(2 * nx, ROWS, qw)
    fin_copies = []
    for n, (d, f) in enumerate(plane):
        other_x, other_role, device = in_plane(d, f)
        fin_copies.append(
            send(mixed.at[other_x * 2 + other_role], final.at[mine], fin_s.at[n], fin_r.at[n], device)
        )
    final[mine] = mixed[mine]
    for copy in fin_copies:
        copy.wait_recv()
    for q in range(4):
        total = None
        for p in range(nx // 2):
            term = final[(2 * p + q // 2) * 2 + q % 2].astype(F32)
            total = term if total is None else total + term
        out[:, q * qw : (q + 1) * qw] = total
    for copy in (
        tab_copies + gath_copies + list(out_copies.values()) + list(live.values())
        + list(back_copies.values()) + fin_copies
    ):
        copy.wait_send()


def experts_of_tokens(normed, table, up_weight, down_weight, nx, nz, capacity, width):
    qw = normed.shape[-1]
    hidden = up_weight.shape[1]
    block = nx * capacity
    chunk = max(1, nz // 4)
    chunks = nz // chunk
    any_space = pl.BlockSpec(memory_space=pl.ANY)
    vmem = pl.BlockSpec(memory_space=pltpu.VMEM)
    dma = pltpu.SemaphoreType.DMA
    return pl.pallas_call(
        functools.partial(moe_kernel, nx, nz, capacity, width, chunk),
        out_shape=jax.ShapeDtypeStruct((ROWS, 4 * qw), F32),
        in_specs=[vmem, vmem, any_space, any_space],
        out_specs=vmem,
        scratch_shapes=[
            pltpu.VMEM((4 * qw, hidden), BF16),
            pltpu.VMEM((hidden, width), BF16),
            pltpu.VMEM((2 * nx, ROWS, qw), BF16),
            pltpu.VMEM((nx, *table.shape[1:]), BF16),
            pltpu.VMEM((nz, block, qw), BF16),
            pltpu.VMEM((4, nz, block, qw), BF16),
            pltpu.VMEM((2, 2, nz, block, qw), BF16),
            pltpu.VMEM((2, nz, block, qw), BF16),
            pltpu.VMEM((nz, block, qw), BF16),
            pltpu.VMEM((nz, block, qw), BF16),
            pltpu.VMEM((nz, block, qw), BF16),
            pltpu.VMEM((nz, block, qw), BF16),
            pltpu.VMEM((2 * nx, ROWS, qw), BF16),
            pltpu.VMEM((2 * nx, ROWS, qw), BF16),
            dma((2,)),
            dma((nx,)), dma((nx,)),
            dma((2 * nx,)), dma((2 * nx,)),
            dma((nz,)), dma((nz,)),
            dma((5, chunks)), dma((5, chunks)),
            dma((nz,)), dma((nz,)),
            dma((2 * nx,)), dma((2 * nx,)),
        ],
        compiler_params=pltpu.CompilerParams(collective_id=0, has_side_effects=True),
        name="experts_of_tokens",
    )(normed, table, up_weight, down_weight)


def slot_tables(route_ids, gate_weights, capacity, nx, nz, lanes):
    pair_count, pick_count = route_ids.shape
    ep = lax.axis_index("ep")
    z, x = ep // nx, ep % nx
    flat = route_ids.reshape(-1)
    count = flat.shape[0]
    index = jnp.arange(count, dtype=jnp.int32)
    same = (flat[:, None] == flat[None, :]) & (index[None, :] < index[:, None])
    slot = jnp.sum(same.astype(jnp.int32), -1)
    offsets, _ = ring_offsets(nz)
    planes = (z + jnp.array(offsets, jnp.int32) + nz) % nz
    experts = (planes[None, :] * (nx // 2) + jnp.arange(nx // 2, dtype=jnp.int32)[:, None]).reshape(-1)
    named = (experts[:, None] == flat[None, :]).astype(F32)
    token = index // pick_count
    per_device = pair_count // 2
    column = x * 2 * ROWS + token // per_device * ROWS + token % per_device
    here = column[:, None] == jnp.arange(lanes, dtype=jnp.int32)[None, :]
    values = jnp.concatenate(
        [
            jnp.where(here, (slot + 1).astype(F32)[:, None], 0.0),
            jnp.where(here, gate_weights.reshape(-1)[:, None], 0.0),
        ],
        axis=1,
    )
    return jnp.dot(named, values).astype(BF16).reshape(nx // 2, nz, 2 * lanes)


def local(
    residual,
    queries,
    key_new,
    value_new,
    key_cache,
    value_cache,
    lengths,
    sink_logits,
    norm_gain,
    route_ids,
    route_logits,
    up_weight,
    down_weight,
):
    context = attention(queries, key_new, value_new, key_cache, value_cache, lengths, sink_logits)
    hidden_state = residual.astype(F32) + context
    normed = (
        hidden_state
        * lax.rsqrt(jnp.mean(hidden_state * hidden_state, -1, keepdims=True) + 1e-05)
        * norm_gain
    ).astype(BF16)
    gate_weights = jax.nn.softmax(route_logits, axis=-1)
    pair_count, pick_count = route_ids.shape
    rank_count = lax.axis_size("ep")
    experts = rank_count // 2
    capacity = min(pair_count, max(2, (pair_count * pick_count + experts - 1) // experts))
    nx = TILE // capacity
    nz = rank_count // nx
    count, width = residual.shape
    qw = -(-width // (4 * 128)) * 128
    lanes = -(-2 * nx * ROWS // 128) * 128
    table = slot_tables(route_ids, gate_weights, capacity, nx, nz, lanes)
    normed = jnp.pad(normed, ((0, ROWS - count), (0, 4 * qw - width)))
    normed = normed.reshape(ROWS, 4, qw).transpose(1, 0, 2)
    expert_out = experts_of_tokens(normed, table, up_weight, down_weight, nx, nz, capacity, width)
    return (hidden_state + expert_out[:count, :width]).astype(BF16)


def solution(mesh):
    placed = (
        P(("groups", "ep", "role"), None),
        P(("groups", "ep", "role"), None),
        P(("groups", "ep", "role"), None),
        P(("groups", "ep", "role"), None),
        P(("groups", "ep", "role"), None, None),
        P(("groups", "ep", "role"), None, None),
        P(("groups", "ep", "role")),
        P(),
        P(),
        P(("groups", "ep"), None),
        P(("groups", "ep"), None),
        P(None, ("ep", "role")),
        P(("ep", "role"), None),
    )
    return jax.shard_map(
        local,
        mesh=mesh,
        in_specs=placed,
        out_specs=P(("groups", "ep", "role"), None),
        check_vma=False,
    )
```

```python
import functools

import jax
import jax.numpy as jnp
from jax import lax
from jax.experimental import pallas as pl
from jax.experimental.pallas import tpu as pltpu
from jax.sharding import PartitionSpec as P

HD = 64
ROWS = 8
TILE = 16
ORDER = "i0 r0 f0 i1 h0 r1 f1 b0 i2 h1 r2 f2 b1 i3 h2 r3 f3 b2 h3 b3"
CHUNKS = [4, 4, 4, 4]
MESH = pl.DeviceIdType.MESH
BF16 = jnp.bfloat16
F32 = jnp.float32


def ring_offsets(n):
    offsets = []
    for d in range(n // 2, 0, -1):
        offsets += [d] if 2 * d == n else [-d, d]
    offsets.append(0)
    opposite = [next(b for b, o in enumerate(offsets) if (o + offsets[a]) % n == 0) for a in range(n)]
    return offsets, opposite


def layer_kernel(
    nx, nz, capacity, picks, chunks, order,
    lengths, residual_hbm, queries_hbm, key_new_hbm, value_new_hbm, key_hbm, value_hbm, sink_hbm, gain_hbm,
    ids_hbm, logits_hbm, up_hbm, down_hbm, out,
    residual_v, queries_v, key_new, value_new, keys, values, sink_v, gain, ids_v, logits_v,
    wide, by_group, by_token, hidden, lanes_v, normed, table,
    up, down, gath, tabs, packed, rows, part, part_in, half_out, half_in, back, returned, mixed, final,
    load_sem, cache_sem, tab_s, tab_r, gath_s, gath_r, out_s, out_r, fwd_s, fwd_r, back_s, back_r, fin_s, fin_r,
):
    ep, role = lax.axis_index("ep"), lax.axis_index("role")
    z, x = ep // nx, ep % nx
    half = x % 2
    mine = x * 2 + role
    quarter = half * 2 + role
    sibling = {"ep": ep, "role": 1 - role}
    pair = {"ep": ep + 1 - 2 * half, "role": role}
    count, width = out.shape
    qw = packed.shape[-1]
    block = nx * capacity
    offsets, opposite = ring_offsets(nz)
    plane = [(d, f) for d in range(nx) for f in range(2) if d or f]

    def in_plane(d, f):
        other_x, other_role = (x + d) % nx, (role + f) % 2
        return other_x, other_role, {"ep": z * nx + other_x, "role": other_role}

    def place(k):
        return (z + offsets[k] + nz) % nz

    def along_z(k):
        return {"ep": place(k) * nx + x, "role": role}

    def send(src, dst, ssem, rsem, device):
        copy = pltpu.make_async_remote_copy(
            src_ref=src, dst_ref=dst, send_sem=ssem, recv_sem=rsem, device_id=device, device_id_type=MESH
        )
        copy.start()
        return copy

    barrier = pltpu.get_barrier_semaphore()
    for d, f in plane:
        pl.semaphore_signal(barrier, inc=1, device_id=in_plane(d, f)[2], device_id_type=MESH)
    for k in range(nz - 1):
        pl.semaphore_signal(barrier, inc=1, device_id=along_z(k), device_id_type=MESH)

    loads = {}
    for n, (name, src, dst) in enumerate((
        ("queries", queries_hbm, queries_v), ("key_new", key_new_hbm, key_new), ("sink", sink_hbm, sink_v),
        ("ids", ids_hbm, ids_v), ("logits", logits_hbm, logits_v), ("value_new", value_new_hbm, value_new),
        ("residual", residual_hbm, residual_v), ("gain", gain_hbm, gain),
        ("up", up_hbm, up), ("down", down_hbm, down),
    )):
        loads[name] = pltpu.make_async_copy(src, dst, load_sem.at[n])
    cache = [
        [pltpu.make_async_copy(src.at[t], dst.at[t], cache_sem.at[i, t]) for t in range(count)]
        for i, (src, dst) in enumerate(((key_hbm, keys), (value_hbm, values)))
    ]
    for name in ("ids", "logits", "queries", "key_new", "sink"):
        loads[name].start()
    for copies in cache:
        for copy in copies:
            copy.start()
    for name in ("value_new", "residual", "gain", "up", "down"):
        loads[name].start()

    lanes = table.shape[-1]
    experts = table.shape[0] * nz
    lane8 = lax.broadcasted_iota(jnp.int32, (8, lanes), 1)
    lanes_v[...] = jnp.zeros(lanes_v.shape, F32)
    loads["ids"].wait()
    loads["logits"].wait()
    tokens_here = ids_v.shape[1]
    lanes_v[0, :picks, :tokens_here] = ids_v[...].astype(F32)
    lanes_v[1, :picks, :tokens_here] = logits_v[...]
    shift = ROWS - count
    filled = (lane8 % ROWS < count) & (lane8 < 2 * ROWS)

    def to_column(block8):
        return jnp.where(lane8 < ROWS, block8, pltpu.roll(block8, shift, 1))

    chosen = jnp.where(filled, to_column(lanes_v[0]), -1.0)
    logit = to_column(lanes_v[1])
    top = logit[0:1]
    for k in range(1, picks):
        top = jnp.maximum(top, logit[k : k + 1])
    raised = jnp.exp(logit - top)
    total = raised[0:1]
    for k in range(1, picks):
        total = total + raised[k : k + 1]
    gate = raised / total
    chosen = pltpu.roll(chosen, x * 2 * ROWS, 1)
    gate = pltpu.roll(gate, x * 2 * ROWS, 1)
    line = lax.broadcasted_iota(jnp.int32, (experts, lanes), 0)
    expert = ((line % nz) * (nx // 2) + line // nz).astype(F32)
    hits = jnp.zeros((experts, lanes), F32)
    weight = jnp.zeros((experts, lanes), F32)
    for k in range(picks):
        is_it = jnp.broadcast_to(chosen[k : k + 1], (experts, lanes)) == expert
        hits = hits + jnp.where(is_it, 1.0, 0.0)
        weight = weight + jnp.where(is_it, jnp.broadcast_to(gate[k : k + 1], (experts, lanes)), 0.0)
    before = lax.broadcasted_iota(jnp.int32, (lanes, lanes), 0) < lax.broadcasted_iota(jnp.int32, (lanes, lanes), 1)
    earlier = jnp.dot(
        hits.astype(BF16), jnp.where(before, 1.0, 0.0).astype(BF16), preferred_element_type=F32
    )
    table[...] = jnp.where(earlier > 0.5, -weight, weight).astype(BF16).reshape(table.shape)

    kv_width = key_new.shape[1]
    heads_kv = kv_width // HD
    heads = width // HD
    group = heads // heads_kv
    lines = by_group.shape[0]
    low = lax.broadcasted_iota(jnp.int32, (ROWS, 128), 1) < HD

    def half_tile(ref_tile, is_high, want_high):
        return ref_tile if is_high == want_high else pltpu.roll(ref_tile, HD, 1)

    last = width - 3 * qw
    clear = last // 128 * 128
    normed[3, :, clear:] = jnp.zeros((ROWS, qw - clear), BF16)
    part[1, 1, :, :, clear:] = jnp.zeros((nz, block, qw - clear), BF16)
    wide[...] = jnp.zeros(wide.shape, F32)
    by_group[group:] = jnp.zeros((lines - group, *by_group.shape[1:]), F32)
    by_token[count:] = jnp.zeros((ROWS - count, *by_token.shape[1:]), F32)
    loads["queries"].wait()
    wide[:count, :width] = queries_v[...].astype(F32)

    def head_tile(h):
        return wide[:, h // 2 * 128 : h // 2 * 128 + 128]

    for g in range(group):
        for m in range(0, heads_kv, 2):
            first, second = m * group + g, (m + 1) * group + g
            value = half_tile(head_tile(first), first % 2, 0)
            if m + 1 < heads_kv:
                value = jnp.where(low, value, half_tile(head_tile(second), second % 2, 1))
                by_group[g, :, m * HD : m * HD + 128] = value
            else:
                by_group[g, :, m * HD : m * HD + HD] = value[:, :HD]
    loads["sink"].wait()
    lanes_v[0, 0:1, :heads] = sink_v[...]
    row = lax.broadcasted_iota(jnp.int32, (heads_kv * lines, lanes), 0)
    col = lax.broadcasted_iota(jnp.int32, (heads_kv * lines, lanes), 1)
    of_head = (row // lines * group + row % lines == col) & (row % lines < group)
    spread = jnp.broadcast_to(lanes_v[0, 0:1, :], (heads_kv * lines, lanes))
    sink = jnp.sum(jnp.where(of_head, spread, 0.0), axis=1, keepdims=True)
    loads["key_new"].wait()
    loads["value_new"].wait()
    fresh_keys, fresh_values = key_new[...].astype(F32), value_new[...].astype(F32)
    kv_of = lax.broadcasted_iota(jnp.int32, (lines, kv_width), 1) // HD
    window = keys.shape[2]
    slot = lax.broadcasted_iota(jnp.int32, (heads_kv * lines, window), 1)
    scale = HD ** (-0.5)
    for t in range(count):
        query = by_group[:, t, :]
        query = jnp.concatenate([jnp.where(kv_of == k, query, 0.0) for k in range(heads_kv)], axis=0)
        cache[0][t].wait()
        cached = jnp.dot(query.astype(BF16), keys[t], preferred_element_type=F32) * scale
        fresh = jnp.sum(query * fresh_keys[t : t + 1], axis=1, keepdims=True) * scale
        length = lengths[t]
        newest = length - 1
        position = newest - jnp.bitwise_and(newest - slot, window - 1)
        visible = (position >= 0) & (position >= length - window + 1)
        cached = jnp.where(visible, cached, -1e30)
        highest = jnp.maximum(jnp.maximum(jnp.max(cached, axis=1, keepdims=True), fresh), sink)
        weights = jnp.exp(cached - highest)
        fresh_weight = jnp.exp(fresh - highest)
        denominator = jnp.sum(weights, axis=1, keepdims=True) + fresh_weight + jnp.exp(sink - highest)
        probs = (weights / denominator).astype(BF16)
        fresh_prob = (fresh_weight / denominator).astype(BF16).astype(F32)
        cache[1][t].wait()
        seen = lax.dot_general(probs, values[t], (((1,), (1,)), ((), ())), preferred_element_type=F32)
        seen = seen + fresh_prob * fresh_values[t : t + 1]
        merged = None
        for k in range(heads_kv):
            term = jnp.where(kv_of == k, seen[k * lines : (k + 1) * lines], 0.0)
            merged = term if merged is None else merged + term
        by_token[t, :, :kv_width] = merged
    loads["residual"].wait()
    wide[:count, :width] = residual_v[...].astype(F32)

    def context_tile(h, want_high):
        g, k = h % group, h // group
        return half_tile(by_token[:, g, k // 2 * 128 : k // 2 * 128 + 128], k % 2, want_high)

    for j in range(wide.shape[1] // 128):
        upper = context_tile(2 * j + 1, 1) if 2 * j + 1 < heads else 0.0
        hidden[:, j * 128 : (j + 1) * 128] = wide[:, j * 128 : (j + 1) * 128] + jnp.where(
            low, context_tile(2 * j, 0), upper
        )
    state = hidden[:, :width]
    inverse = lax.rsqrt(jnp.sum(state * state, axis=1, keepdims=True) * (1.0 / width) + 1e-05)
    loads["gain"].wait()
    for q in range(4):
        w = min(qw, width - q * qw)
        cut = slice(q * qw, q * qw + w)
        normed[q, :, :w] = (hidden[:, cut] * inverse * gain[:, cut]).astype(BF16)

    pl.semaphore_wait(barrier, len(plane) + nz - 1)

    tab_copies, gath_copies = [], []
    for n, (d, f) in enumerate(plane):
        other_x, other_role, device = in_plane(d, f)
        if f == 0:
            tab_copies.append(send(table.at[other_x // 2], tabs.at[x], tab_s.at[d], tab_r.at[d], device))
        wanted = (other_x % 2) * 2 + other_role
        gath_copies.append(send(normed.at[wanted], gath.at[mine], gath_s.at[n], gath_r.at[n], device))
    gath[mine] = normed[quarter]
    tabs[x] = table[x // 2]
    for copy in tab_copies:
        copy.wait_recv()
    codes = jnp.sum(tabs[...].astype(F32), axis=0)
    row = lax.broadcasted_iota(jnp.int32, (nz, block, lanes), 1)
    col = lax.broadcasted_iota(jnp.int32, (nz, block, lanes), 2)
    codes = jnp.broadcast_to(codes[:, None, :], (nz, block, lanes))
    signed = jnp.where(row % capacity == 0, codes, -codes)
    hit = (col // (2 * ROWS) == row // capacity) & (signed > 0.0)
    choose = jnp.where(hit, 1.0, 0.0).astype(BF16).reshape(nz * block, lanes)
    blend = jnp.where(hit, signed, 0.0).astype(BF16).reshape(nz * block, lanes)
    for copy in gath_copies:
        copy.wait_recv()
    tokens = gath[...].reshape(2 * nx * ROWS, qw)
    if tokens.shape[0] < lanes:
        tokens = jnp.concatenate([tokens, jnp.zeros((lanes - tokens.shape[0], qw), BF16)], axis=0)
    packed[...] = jnp.dot(choose, tokens, preferred_element_type=F32).astype(BF16).reshape(nz, block, qw)

    out_copies = {}
    for k in range(nz - 1):
        to = opposite[k]
        out_copies[k] = send(packed.at[place(k)], rows.at[quarter, to], out_s.at[k], out_r.at[to], along_z(k))
    rows[quarter, nz - 1] = packed[z]
    back_copies = {}
    live = {}
    starts = [sum(chunks[:c]) for c in range(len(chunks))]

    def span(c):
        return pl.ds(starts[c], chunks[c])

    def blocks(c):
        return range(starts[c], starts[c] + chunks[c])

    def stage_in(c):
        for k in blocks(c):
            if k < nz - 1:
                out_copies[opposite[k]].wait_recv()
            one = rows.at[quarter, k]
            live["pair", k] = send(one, one, fwd_s.at[0, k], fwd_r.at[0, k], pair)
        mine_rows = rows.at[quarter, span(c)]
        live["sib", c] = send(mine_rows, mine_rows, fwd_s.at[1, c], fwd_r.at[1, c], sibling)

    def stage_relay(c):
        for k in blocks(c):
            live["pair", k].wait_recv()
        their_rows = rows.at[(1 - half) * 2 + role, span(c)]
        live["relay", c] = send(their_rows, their_rows, fwd_s.at[2, c], fwd_r.at[2, c], sibling)

    def stage_ffn(c):
        live["sib", c].wait_recv()
        live["relay", c].wait_recv()
        if c == 0:
            loads["up"].wait()
        at = slice(starts[c], starts[c] + chunks[c])
        total = None
        for q in range(4):
            w = min(qw, width - q * qw)
            piece = rows[q, at, :, :w].reshape(chunks[c] * block, w)
            term = lax.dot_general(
                piece, up[:, q * qw : q * qw + w], (((1,), (1,)), ((), ())), preferred_element_type=F32
            )
            total = term if total is None else total + term
        active = (total / (1.0 + jnp.exp(-total))).astype(BF16)
        if c == 0:
            loads["down"].wait()
        for q in range(4):
            w = min(qw, width - q * qw)
            value = jnp.dot(active, down[:, q * qw : q * qw + w], preferred_element_type=F32).astype(BF16)
            part[q // 2, q % 2, at, :, :w] = value.reshape(chunks[c], block, w)
        live["part", c] = send(
            part.at[:, 1 - role, span(c)], part_in.at[:, span(c)], fwd_s.at[3, c], fwd_r.at[3, c], sibling
        )

    def stage_half(c):
        live["part", c].wait_recv()
        at = slice(starts[c], starts[c] + chunks[c])
        half_out[at] = (part[1 - half, role, at].astype(F32) + part_in[1 - half, at].astype(F32)).astype(BF16)
        for k in blocks(c):
            live["half", k] = send(half_out.at[k], half_in.at[k], fwd_s.at[4, k], fwd_r.at[4, k], pair)

    def stage_back(c):
        for k in blocks(c):
            live["half", k].wait_recv()
            back[k] = (
                part[half, role, k].astype(F32) + part_in[half, k].astype(F32) + half_in[k].astype(F32)
            ).astype(BF16)
            if k == nz - 1:
                returned[z] = back[k]
            else:
                back_copies[k] = send(
                    back.at[k], returned.at[z], back_s.at[k], back_r.at[opposite[k]], along_z(k)
                )

    stages = {"i": stage_in, "r": stage_relay, "f": stage_ffn, "h": stage_half, "b": stage_back}
    for step in order.split():
        stages[step[0]](int(step[1:]))

    for k in range(nz - 1):
        back_copies[opposite[k]].wait_recv()
    mix = lax.dot_general(
        blend, returned[...].reshape(nz * block, qw), (((0,), (0,)), ((), ())), preferred_element_type=F32
    )
    mixed[...] = mix[: 2 * nx * ROWS].astype(BF16).reshape(2 * nx, ROWS, qw)
    fin_copies = []
    for n, (d, f) in enumerate(plane):
        other_x, other_role, device = in_plane(d, f)
        fin_copies.append(
            send(mixed.at[other_x * 2 + other_role], final.at[mine], fin_s.at[n], fin_r.at[n], device)
        )
    final[mine] = mixed[mine]
    for copy in fin_copies:
        copy.wait_recv()
    for q in range(4):
        total = None
        for p in range(nx // 2):
            term = final[(2 * p + q // 2) * 2 + q % 2].astype(F32)
            total = term if total is None else total + term
        w = min(qw, width - q * qw)
        cut = slice(q * qw, q * qw + w)
        out[:, cut] = (hidden[:count, cut] + total[:count, :w]).astype(BF16)
    for copy in (
        tab_copies + gath_copies + list(out_copies.values()) + list(live.values())
        + list(back_copies.values()) + fin_copies
    ):
        copy.wait_send()


def local(
    residual,
    queries,
    key_new,
    value_new,
    key_cache,
    value_cache,
    lengths,
    sink_logits,
    norm_gain,
    route_ids,
    route_logits,
    up_weight,
    down_weight,
):
    pair_count, picks = route_ids.shape
    rank_count = lax.axis_size("ep")
    experts = rank_count // 2
    capacity = min(pair_count, max(2, (pair_count * picks + experts - 1) // experts))
    nx = TILE // capacity
    nz = rank_count // nx
    count, width = residual.shape
    window, kv_width = key_cache.shape[1:]
    heads_kv = kv_width // HD
    group = width // kv_width
    lines = -(-group // 16) * 16
    hidden_units = up_weight.shape[1]
    qw = -(-width // (4 * 128)) * 128
    padded = -(-width // 128) * 128
    lanes = 128
    block = nx * capacity
    chunks = CHUNKS if sum(CHUNKS) == nz else [nz]
    order = ORDER if sum(CHUNKS) == nz else "i0 r0 f0 h0 b0"
    dma = pltpu.SemaphoreType.DMA
    any_space = pl.BlockSpec(memory_space=pl.ANY)

    def vmem(*shape, dtype=BF16):
        return pltpu.VMEM(shape, dtype)

    return pl.pallas_call(
        functools.partial(layer_kernel, nx, nz, capacity, picks, chunks, order),
        out_shape=jax.ShapeDtypeStruct((count, width), BF16),
        in_specs=[pl.BlockSpec(memory_space=pltpu.SMEM)] + [any_space] * 12,
        out_specs=pl.BlockSpec(memory_space=pltpu.VMEM),
        scratch_shapes=[
            vmem(count, width),
            vmem(count, width),
            vmem(count, kv_width),
            vmem(count, kv_width),
            vmem(count, kv_width, window),
            vmem(count, kv_width, window),
            vmem(1, sink_logits.shape[0], dtype=F32),
            vmem(1, width, dtype=F32),
            vmem(picks, pair_count, dtype=jnp.int32),
            vmem(picks, pair_count, dtype=F32),
            vmem(ROWS, padded, dtype=F32),
            vmem(lines, ROWS, kv_width, dtype=F32),
            vmem(ROWS, lines, -(-kv_width // 128) * 128, dtype=F32),
            vmem(ROWS, padded, dtype=F32),
            vmem(2, 8, lanes, dtype=F32),
            vmem(4, ROWS, qw),
            vmem(nx // 2, nz, lanes),
            vmem(hidden_units, width),
            vmem(hidden_units, width),
            vmem(2 * nx, ROWS, qw),
            vmem(nx, nz, lanes),
            vmem(nz, block, qw),
            vmem(4, nz, block, qw),
            vmem(2, 2, nz, block, qw),
            vmem(2, nz, block, qw),
            vmem(nz, block, qw),
            vmem(nz, block, qw),
            vmem(nz, block, qw),
            vmem(nz, block, qw),
            vmem(2 * nx, ROWS, qw),
            vmem(2 * nx, ROWS, qw),
            dma((10,)),
            dma((2, count)),
            dma((nx,)), dma((nx,)),
            dma((2 * nx,)), dma((2 * nx,)),
            dma((nz,)), dma((nz,)),
            dma((5, nz)), dma((5, nz)),
            dma((nz,)), dma((nz,)),
            dma((2 * nx,)), dma((2 * nx,)),
        ],
        compiler_params=pltpu.CompilerParams(collective_id=0, has_side_effects=True),
        name="layer",
    )(
        lengths, residual, queries, key_new, value_new,
        key_cache.transpose(0, 2, 1), value_cache.transpose(0, 2, 1),
        sink_logits.reshape(1, -1), norm_gain.reshape(1, -1), route_ids.T, route_logits.T,
        up_weight.T, down_weight,
    )


def solution(mesh):
    placed = (
        P(("groups", "ep", "role"), None),
        P(("groups", "ep", "role"), None),
        P(("groups", "ep", "role"), None),
        P(("groups", "ep", "role"), None),
        P(("groups", "ep", "role"), None, None),
        P(("groups", "ep", "role"), None, None),
        P(("groups", "ep", "role")),
        P(),
        P(),
        P(("groups", "ep"), None),
        P(("groups", "ep"), None),
        P(None, ("ep", "role")),
        P(("ep", "role"), None),
    )
    return jax.shard_map(
        local,
        mesh=mesh,
        in_specs=placed,
        out_specs=P(("groups", "ep", "role"), None),
        check_vma=False,
    )
```

```python
import functools

import jax
import jax.numpy as jnp
from jax import lax
from jax.experimental import pallas as pl
from jax.experimental.pallas import tpu as pltpu
from jax.sharding import PartitionSpec as P

HD = 64
ROWS = 8
TILE = 16
ORDER = ("i0 r0 i1 f0", "i2 h0 r1 f1", "b0 h1 i3 r2", "f2 b1 r3 h2", "f3 b2 h3 b3")
CHUNKS = [2, 3, 5, 6]
MESH = pl.DeviceIdType.MESH
BF16 = jnp.bfloat16
F32 = jnp.float32


def ring_offsets(n):
    offsets = []
    for d in range(n // 2, 0, -1):
        offsets += [d] if 2 * d == n else [-d, d]
    offsets.append(0)
    opposite = [next(b for b, o in enumerate(offsets) if (o + offsets[a]) % n == 0) for a in range(n)]
    return offsets, opposite


def layer_kernel(
    nx, nz, capacity, picks, chunks, order,
    lengths, residual_hbm, queries_hbm, key_new_hbm, value_new_hbm, key_hbm, value_hbm, sink_hbm, gain_hbm,
    ids_hbm, logits_hbm, up_hbm, down_hbm, out,
    residual_v, queries_v, key_new, value_new, keys, values, sink_v, gain, ids_v, logits_v,
    wide, by_group, by_token, hidden, lanes_v, normed, table,
    up, down, up4, down4, gath, tabs, packed, rows, part, part_in, half_out, half_in, back, returned, mixed, final,
    load_sem, cache_sem, tab_s, tab_r, gath_s, gath_r, out_s, out_r, fwd_s, fwd_r, back_s, back_r, fin_s, fin_r,
):
    ep, role = lax.axis_index("ep"), lax.axis_index("role")
    z, x = ep // nx, ep % nx
    half = x % 2
    mine = x * 2 + role
    quarter = half * 2 + role
    sibling = {"ep": ep, "role": 1 - role}
    pair = {"ep": ep + 1 - 2 * half, "role": role}
    count, width = out.shape
    qw = packed.shape[-1]
    block = nx * capacity
    offsets, opposite = ring_offsets(nz)
    plane = [(d, f) for d in range(nx) for f in range(2) if d or f]

    def in_plane(d, f):
        other_x, other_role = (x + d) % nx, (role + f) % 2
        return other_x, other_role, {"ep": z * nx + other_x, "role": other_role}

    def place(k):
        return (z + offsets[k] + nz) % nz

    def along_z(k):
        return {"ep": place(k) * nx + x, "role": role}

    def send(src, dst, ssem, rsem, device):
        copy = pltpu.make_async_remote_copy(
            src_ref=src, dst_ref=dst, send_sem=ssem, recv_sem=rsem, device_id=device, device_id_type=MESH
        )
        copy.start()
        return copy

    barrier = pltpu.get_barrier_semaphore()
    for d, f in plane:
        pl.semaphore_signal(barrier, inc=1, device_id=in_plane(d, f)[2], device_id_type=MESH)
    for k in range(nz - 1):
        pl.semaphore_signal(barrier, inc=1, device_id=along_z(k), device_id_type=MESH)

    loads = {}
    for n, (name, src, dst) in enumerate((
        ("queries", queries_hbm, queries_v), ("key_new", key_new_hbm, key_new), ("sink", sink_hbm, sink_v),
        ("ids", ids_hbm, ids_v), ("logits", logits_hbm, logits_v), ("value_new", value_new_hbm, value_new),
        ("residual", residual_hbm, residual_v), ("gain", gain_hbm, gain),
        ("up", up_hbm, up), ("down", down_hbm, down),
    )):
        loads[name] = pltpu.make_async_copy(src, dst, load_sem.at[n])
    cache = [
        [pltpu.make_async_copy(src.at[t], dst.at[t], cache_sem.at[i, t]) for t in range(count)]
        for i, (src, dst) in enumerate(((key_hbm, keys), (value_hbm, values)))
    ]
    early = ("queries", "ids", "logits", "key_new", "sink", "value_new", "residual", "gain")
    for name in early:
        loads[name].start()
    for copies in cache:
        for copy in copies:
            copy.start()
    for name in ("up", "down"):
        loads[name].start()

    lanes = table.shape[-1]
    experts = table.shape[0] * nz
    lane8 = lax.broadcasted_iota(jnp.int32, (8, lanes), 1)
    lanes_v[...] = jnp.zeros(lanes_v.shape, F32)
    normed[3] = jnp.zeros((ROWS, qw), BF16)
    wide[...] = jnp.zeros(wide.shape, F32)
    heads_kv = key_new.shape[1] // HD
    group = width // HD // heads_kv
    by_group[group:] = jnp.zeros((by_group.shape[0] - group, *by_group.shape[1:]), F32)
    by_token[count:] = jnp.zeros((ROWS - count, *by_token.shape[1:]), F32)
    for name in early:
        loads[name].wait()
    tokens_here = ids_v.shape[1]
    lanes_v[0, :picks, :tokens_here] = ids_v[...].astype(F32)
    lanes_v[1, :picks, :tokens_here] = logits_v[...]
    shift = ROWS - count
    filled = (lane8 % ROWS < count) & (lane8 < 2 * ROWS)

    def to_column(block8):
        return jnp.where(lane8 < ROWS, block8, pltpu.roll(block8, shift, 1))

    chosen = jnp.where(filled, to_column(lanes_v[0]), -1.0)
    logit = to_column(lanes_v[1])
    top = logit[0:1]
    for k in range(1, picks):
        top = jnp.maximum(top, logit[k : k + 1])
    raised = jnp.exp(logit - top)
    total = raised[0:1]
    for k in range(1, picks):
        total = total + raised[k : k + 1]
    gate = raised / total
    chosen = pltpu.roll(chosen, x * 2 * ROWS, 1)
    gate = pltpu.roll(gate, x * 2 * ROWS, 1)
    line = lax.broadcasted_iota(jnp.int32, (experts, lanes), 0)
    expert = ((line % nz) * (nx // 2) + line // nz).astype(F32)
    hits = jnp.zeros((experts, lanes), F32)
    weight = jnp.zeros((experts, lanes), F32)
    for k in range(picks):
        is_it = jnp.broadcast_to(chosen[k : k + 1], (experts, lanes)) == expert
        hits = hits + jnp.where(is_it, 1.0, 0.0)
        weight = weight + jnp.where(is_it, jnp.broadcast_to(gate[k : k + 1], (experts, lanes)), 0.0)
    before = lax.broadcasted_iota(jnp.int32, (lanes, lanes), 0) < lax.broadcasted_iota(jnp.int32, (lanes, lanes), 1)
    earlier = jnp.dot(
        hits.astype(BF16), jnp.where(before, 1.0, 0.0).astype(BF16), preferred_element_type=F32
    )
    table[...] = jnp.where(earlier > 0.5, -weight, weight).astype(BF16).reshape(table.shape)

    kv_width = key_new.shape[1]
    heads = width // HD
    lines = by_group.shape[0]
    low = lax.broadcasted_iota(jnp.int32, (ROWS, 128), 1) < HD

    def half_tile(ref_tile, is_high, want_high):
        return ref_tile if is_high == want_high else pltpu.roll(ref_tile, HD, 1)

    wide[:count, :width] = queries_v[...].astype(F32)

    def head_tile(h):
        return wide[:, h // 2 * 128 : h // 2 * 128 + 128]

    for g in range(group):
        for m in range(0, heads_kv, 2):
            first, second = m * group + g, (m + 1) * group + g
            value = half_tile(head_tile(first), first % 2, 0)
            if m + 1 < heads_kv:
                value = jnp.where(low, value, half_tile(head_tile(second), second % 2, 1))
                by_group[g, :, m * HD : m * HD + 128] = value
            else:
                by_group[g, :, m * HD : m * HD + HD] = value[:, :HD]
    lanes_v[0, 0:1, :heads] = sink_v[...]
    row = lax.broadcasted_iota(jnp.int32, (heads_kv * lines, lanes), 0)
    col = lax.broadcasted_iota(jnp.int32, (heads_kv * lines, lanes), 1)
    of_head = (row // lines * group + row % lines == col) & (row % lines < group)
    spread = jnp.broadcast_to(lanes_v[0, 0:1, :], (heads_kv * lines, lanes))
    sink = jnp.sum(jnp.where(of_head, spread, 0.0), axis=1, keepdims=True)
    fresh_keys, fresh_values = key_new[...].astype(F32), value_new[...].astype(F32)
    kv_of = lax.broadcasted_iota(jnp.int32, (lines, kv_width), 1) // HD
    window = keys.shape[2]
    slot = lax.broadcasted_iota(jnp.int32, (heads_kv * lines, window), 1)
    scale = HD ** (-0.5)
    for copy in cache[0]:
        copy.wait()
    scores, fresh_scores, seen = [], [], []
    for t in range(count):
        query = by_group[:, t, :]
        query = jnp.concatenate([jnp.where(kv_of == k, query, 0.0) for k in range(heads_kv)], axis=0)
        scores.append(jnp.dot(query.astype(BF16), keys[t], preferred_element_type=F32) * scale)
        fresh_scores.append(jnp.sum(query * fresh_keys[t : t + 1], axis=1, keepdims=True) * scale)
    for copy in cache[1]:
        copy.wait()
    for t in range(count):
        fresh = fresh_scores[t]
        length = lengths[t]
        newest = length - 1
        position = newest - jnp.bitwise_and(newest - slot, window - 1)
        visible = (position >= 0) & (position >= length - window + 1)
        cached = jnp.where(visible, scores[t], -1e30)
        highest = jnp.maximum(jnp.maximum(jnp.max(cached, axis=1, keepdims=True), fresh), sink)
        weights = jnp.exp(cached - highest)
        fresh_weight = jnp.exp(fresh - highest)
        denominator = jnp.sum(weights, axis=1, keepdims=True) + fresh_weight + jnp.exp(sink - highest)
        probs = (weights / denominator).astype(BF16)
        fresh_prob = (fresh_weight / denominator).astype(BF16).astype(F32)
        out_t = lax.dot_general(probs, values[t], (((1,), (1,)), ((), ())), preferred_element_type=F32)
        seen.append(out_t + fresh_prob * fresh_values[t : t + 1])
    for t in range(count):
        merged = None
        for k in range(heads_kv):
            term = jnp.where(kv_of == k, seen[t][k * lines : (k + 1) * lines], 0.0)
            merged = term if merged is None else merged + term
        by_token[t, :, :kv_width] = merged
    wide[:count, :width] = residual_v[...].astype(F32)

    def context_tile(h, want_high):
        g, k = h % group, h // group
        return half_tile(by_token[:, g, k // 2 * 128 : k // 2 * 128 + 128], k % 2, want_high)

    for j in range(wide.shape[1] // 128):
        upper = context_tile(2 * j + 1, 1) if 2 * j + 1 < heads else 0.0
        hidden[:, j * 128 : (j + 1) * 128] = wide[:, j * 128 : (j + 1) * 128] + jnp.where(
            low, context_tile(2 * j, 0), upper
        )
    state = hidden[:, :width]
    inverse = lax.rsqrt(jnp.sum(state * state, axis=1, keepdims=True) * (1.0 / width) + 1e-05)
    for q in range(4):
        w = min(qw, width - q * qw)
        cut = slice(q * qw, q * qw + w)
        normed[q, :, :w] = (hidden[:, cut] * inverse * gain[:, cut]).astype(BF16)

    pl.semaphore_wait(barrier, len(plane) + nz - 1)

    tab_copies, gath_copies = [], []
    for n, (d, f) in enumerate(plane):
        other_x, other_role, device = in_plane(d, f)
        if f == 0:
            tab_copies.append(send(table.at[other_x // 2], tabs.at[x], tab_s.at[d], tab_r.at[d], device))
        wanted = (other_x % 2) * 2 + other_role
        gath_copies.append(send(normed.at[wanted], gath.at[mine], gath_s.at[n], gath_r.at[n], device))
    gath[mine] = normed[quarter]
    tabs[x] = table[x // 2]
    loads["up"].wait()
    loads["down"].wait()
    for stored, whole in ((up4, up), (down4, down)):
        for q in range(4):
            w = min(qw, width - q * qw)
            if w < qw:
                stored[q, :, w // 128 * 128 :] = jnp.zeros((whole.shape[0], qw - w // 128 * 128), BF16)
            stored[q, :, :w] = whole[:, q * qw : q * qw + w]
    for copy in tab_copies:
        copy.wait_recv()
    codes = jnp.sum(tabs[...].astype(F32), axis=0)
    row = lax.broadcasted_iota(jnp.int32, (nz, block, lanes), 1)
    col = lax.broadcasted_iota(jnp.int32, (nz, block, lanes), 2)
    codes = jnp.broadcast_to(codes[:, None, :], (nz, block, lanes))
    signed = jnp.where(row % capacity == 0, codes, -codes)
    hit = (col // (2 * ROWS) == row // capacity) & (signed > 0.0)
    choose = jnp.where(hit, 1.0, 0.0).astype(BF16).reshape(nz * block, lanes)
    blend = jnp.where(hit, signed, 0.0).astype(BF16).reshape(nz * block, lanes)
    for copy in gath_copies:
        copy.wait_recv()
    tokens = gath[...].reshape(2 * nx * ROWS, qw)
    if tokens.shape[0] < lanes:
        tokens = jnp.concatenate([tokens, jnp.zeros((lanes - tokens.shape[0], qw), BF16)], axis=0)
    packed[...] = jnp.dot(choose, tokens, preferred_element_type=F32).astype(BF16).reshape(nz, block, qw)

    out_copies = {}
    for k in range(nz - 1):
        to = opposite[k]
        out_copies[k] = send(packed.at[place(k)], rows.at[quarter, to], out_s.at[k], out_r.at[to], along_z(k))
    rows[quarter, nz - 1] = packed[z]
    back_copies = {}
    live, totals = {}, {}
    starts = [sum(chunks[:c]) for c in range(len(chunks))]

    def span(c):
        return pl.ds(starts[c], chunks[c])

    def blocks(c):
        return range(starts[c], starts[c] + chunks[c])

    def up_dot(c, q):
        piece = rows[q, slice(starts[c], starts[c] + chunks[c])].reshape(chunks[c] * block, qw)
        return lax.dot_general(piece, up4[q], (((1,), (1,)), ((), ())), preferred_element_type=F32)

    def stage_in(c):
        for k in blocks(c):
            if k < nz - 1:
                out_copies[opposite[k]].wait_recv()
            one = rows.at[quarter, k]
            live["pair", k] = send(one, one, fwd_s.at[0, k], fwd_r.at[0, k], pair)
        mine_rows = rows.at[quarter, span(c)]
        live["sib", c] = send(mine_rows, mine_rows, fwd_s.at[1, c], fwd_r.at[1, c], sibling)
        totals[c] = up_dot(c, quarter)

    def stage_relay(c):
        for k in blocks(c):
            live["pair", k].wait_recv()
        their_rows = rows.at[(1 - half) * 2 + role, span(c)]
        live["relay", c] = send(their_rows, their_rows, fwd_s.at[2, c], fwd_r.at[2, c], sibling)
        live["sib", c].wait_recv()
        totals[c] = totals[c] + up_dot(c, half * 2 + 1 - role) + up_dot(c, (1 - half) * 2 + role)

    def stage_ffn(c):
        live["relay", c].wait_recv()
        at = slice(starts[c], starts[c] + chunks[c])
        total = totals[c] + up_dot(c, (1 - half) * 2 + 1 - role)
        active = (total / (1.0 + jnp.exp(-total))).astype(BF16)
        for r in (1 - role, role):
            for h in range(2):
                value = jnp.dot(active, down4[h * 2 + r], preferred_element_type=F32).astype(BF16)
                part[h, r, at] = value.reshape(chunks[c], block, qw)
            if r is not role:
                live["part", c] = send(
                    part.at[:, 1 - role, span(c)], part_in.at[:, span(c)], fwd_s.at[3, c], fwd_r.at[3, c], sibling
                )

    def stage_half(c):
        live["part", c].wait_recv()
        at = slice(starts[c], starts[c] + chunks[c])
        half_out[at] = (part[1 - half, role, at].astype(F32) + part_in[1 - half, at].astype(F32)).astype(BF16)
        for k in blocks(c):
            live["half", k] = send(half_out.at[k], half_in.at[k], fwd_s.at[4, k], fwd_r.at[4, k], pair)

    def stage_back(c):
        for k in blocks(c):
            live["half", k].wait_recv()
            back[k] = (
                part[half, role, k].astype(F32) + part_in[half, k].astype(F32) + half_in[k].astype(F32)
            ).astype(BF16)
            if k == nz - 1:
                returned[z] = back[k]
            else:
                back_copies[k] = send(
                    back.at[k], returned.at[z], back_s.at[k], back_r.at[opposite[k]], along_z(k)
                )

    stages = {"i": stage_in, "r": stage_relay, "f": stage_ffn, "h": stage_half, "b": stage_back}
    for step in " ".join(order).split():
        stages[step[0]](int(step[1:]))

    for k in range(nz - 1):
        back_copies[opposite[k]].wait_recv()
    mix = lax.dot_general(
        blend, returned[...].reshape(nz * block, qw), (((0,), (0,)), ((), ())), preferred_element_type=F32
    )
    mixed[...] = mix[: 2 * nx * ROWS].astype(BF16).reshape(2 * nx, ROWS, qw)
    fin_copies = []
    for n, (d, f) in enumerate(plane):
        other_x, other_role, device = in_plane(d, f)
        fin_copies.append(
            send(mixed.at[other_x * 2 + other_role], final.at[mine], fin_s.at[n], fin_r.at[n], device)
        )
    final[mine] = mixed[mine]
    for copy in fin_copies:
        copy.wait_recv()
    for q in range(4):
        total = None
        for p in range(nx // 2):
            term = final[(2 * p + q // 2) * 2 + q % 2].astype(F32)
            total = term if total is None else total + term
        w = min(qw, width - q * qw)
        cut = slice(q * qw, q * qw + w)
        out[:, cut] = (hidden[:count, cut] + total[:count, :w]).astype(BF16)
    for copy in (
        tab_copies + gath_copies + list(out_copies.values()) + list(live.values())
        + list(back_copies.values()) + fin_copies
    ):
        copy.wait_send()


def local(
    residual,
    queries,
    key_new,
    value_new,
    key_cache,
    value_cache,
    lengths,
    sink_logits,
    norm_gain,
    route_ids,
    route_logits,
    up_weight,
    down_weight,
):
    pair_count, picks = route_ids.shape
    rank_count = lax.axis_size("ep")
    experts = rank_count // 2
    capacity = min(pair_count, max(2, (pair_count * picks + experts - 1) // experts))
    nx = TILE // capacity
    nz = rank_count // nx
    count, width = residual.shape
    window, kv_width = key_cache.shape[1:]
    heads_kv = kv_width // HD
    group = width // kv_width
    lines = -(-group // 16) * 16
    hidden_units = up_weight.shape[1]
    qw = -(-width // (4 * 128)) * 128
    padded = -(-width // 128) * 128
    lanes = 128
    block = nx * capacity
    chunks = CHUNKS if sum(CHUNKS) == nz else [nz]
    order = ORDER if sum(CHUNKS) == nz else ("i0 r0 f0", "h0 b0")
    dma = pltpu.SemaphoreType.DMA
    any_space = pl.BlockSpec(memory_space=pl.ANY)

    def vmem(*shape, dtype=BF16):
        return pltpu.VMEM(shape, dtype)

    return pl.pallas_call(
        functools.partial(layer_kernel, nx, nz, capacity, picks, chunks, order),
        out_shape=jax.ShapeDtypeStruct((count, width), BF16),
        in_specs=[pl.BlockSpec(memory_space=pltpu.SMEM)] + [any_space] * 12,
        out_specs=pl.BlockSpec(memory_space=pltpu.VMEM),
        scratch_shapes=[
            vmem(count, width),
            vmem(count, width),
            vmem(count, kv_width),
            vmem(count, kv_width),
            vmem(count, kv_width, window),
            vmem(count, kv_width, window),
            vmem(1, sink_logits.shape[0], dtype=F32),
            vmem(1, width, dtype=F32),
            vmem(picks, pair_count, dtype=jnp.int32),
            vmem(picks, pair_count, dtype=F32),
            vmem(ROWS, padded, dtype=F32),
            vmem(lines, ROWS, kv_width, dtype=F32),
            vmem(ROWS, lines, -(-kv_width // 128) * 128, dtype=F32),
            vmem(ROWS, padded, dtype=F32),
            vmem(2, 8, lanes, dtype=F32),
            vmem(4, ROWS, qw),
            vmem(nx // 2, nz, lanes),
            vmem(hidden_units, width),
            vmem(hidden_units, width),
            vmem(4, hidden_units, qw),
            vmem(4, hidden_units, qw),
            vmem(2 * nx, ROWS, qw),
            vmem(nx, nz, lanes),
            vmem(nz, block, qw),
            vmem(4, nz, block, qw),
            vmem(2, 2, nz, block, qw),
            vmem(2, nz, block, qw),
            vmem(nz, block, qw),
            vmem(nz, block, qw),
            vmem(nz, block, qw),
            vmem(nz, block, qw),
            vmem(2 * nx, ROWS, qw),
            vmem(2 * nx, ROWS, qw),
            dma((10,)),
            dma((2, count)),
            dma((nx,)), dma((nx,)),
            dma((2 * nx,)), dma((2 * nx,)),
            dma((nz,)), dma((nz,)),
            dma((5, nz)), dma((5, nz)),
            dma((nz,)), dma((nz,)),
            dma((2 * nx,)), dma((2 * nx,)),
        ],
        compiler_params=pltpu.CompilerParams(collective_id=0, has_side_effects=True),
        name="layer",
    )(
        lengths, residual, queries, key_new, value_new,
        key_cache.transpose(0, 2, 1), value_cache.transpose(0, 2, 1),
        sink_logits.reshape(1, -1), norm_gain.reshape(1, -1), route_ids.T, route_logits.T,
        up_weight.T, down_weight,
    )


def solution(mesh):
    placed = (
        P(("groups", "ep", "role"), None),
        P(("groups", "ep", "role"), None),
        P(("groups", "ep", "role"), None),
        P(("groups", "ep", "role"), None),
        P(("groups", "ep", "role"), None, None),
        P(("groups", "ep", "role"), None, None),
        P(("groups", "ep", "role")),
        P(),
        P(),
        P(("groups", "ep"), None),
        P(("groups", "ep"), None),
        P(None, ("ep", "role")),
        P(("ep", "role"), None),
    )
    return jax.shard_map(
        local,
        mesh=mesh,
        in_specs=placed,
        out_specs=P(("groups", "ep", "role"), None),
        check_vma=False,
    )
```
